32 devices in a mesh: corner: 2 (over y), gx: 16 (over z, x, core).
Axes of the slice: x: 2, y: 2, z: 4, core: 2. Of those that a mesh axis runs over, the one named last changes fastest.
Arguments:
- forward_field: float32 [6, 256, 32, 128], P(None, ('corner', 'gx')), parts along dimension 1, may hold values from -180 to 180, as said below
- adjoint_field: float32 [6, 256, 32, 128], P(None, ('corner', 'gx')), parts along dimension 1, may hold values from -6 to 6
- level_set: float32 [128, 32, 128], P('gx'), may hold values from -8 to 8
- region_labels: int32 [128, 32, 128], P('gx'), may hold values from 0 to 3
- upwind_signs: int32 [3, 128, 32, 128], P(None, 'gx'), may hold values from -1 to 1, as said below
- contrast: float32 [8], P('corner'), parts along dimension 0, may hold values from -3 to 3
- line_decay: float32 [32, 128], replicated, may hold values from 0.00078125 to 0.0625
Outputs:
- moved: float32 [256, 32, 128], P(('corner', 'gx')), parts along dimension 0
- speed: float32 [256, 32, 128], P(('corner', 'gx')), parts along dimension 0
The draws below stay inside these ranges and needn't reach their ends.
There are 2 independent parts, one for each index of `corner`. The reference program is written for one: setup_inputs(seed, part) draws one part's arguments, and reference() takes and returns one part's arrays. A program takes and returns all parts, laid end to end along the dimension named above; an argument that names none is the same for every part. Nothing has to cross between parts.
Inputs may be any that keep to these rules, and one draw needn't show every extreme that they name: `forward_field`: forward field of each cell. `upwind_signs`: upwind sign of each cell along each of the three dimensions.
All inputs are finite; a program needn't handle non-finite values.
Results may differ from the reference program's by a relative error of at most 0.0003.
Values sent between devices are 32-bit elements; how exact they have to be, the bound alone decides.
A program may use at most 64 MiB of HBM per device.

```python
import math
import jax
import jax.numpy as jnp
from jax import lax

SPAN_COUNT_DEPTH = 32
SPAN_COUNT_HEIGHT = 128
ITERS = 2
REGIONS = 4
SPAN_COUNT_WIDTH = 128


def draw_forward_field(key, part):
    first_key, second_key = jax.random.split(key)
    shape = (6, SPAN_COUNT_WIDTH, SPAN_COUNT_DEPTH, SPAN_COUNT_HEIGHT)
    positions = jnp.arange(SPAN_COUNT_WIDTH, dtype=jnp.float32) / SPAN_COUNT_WIDTH
    base = jnp.clip(jax.random.normal(first_key, shape, jnp.float32), -6.0, 6.0)
    ramp = 3.0 ** (0.5 * positions)
    rows = jnp.exp(jax.random.uniform(second_key, (1, SPAN_COUNT_WIDTH, SPAN_COUNT_DEPTH, 1), jnp.float32, 0.0, math.log(10.0)))
    return base * ramp[None, :, None, None] * rows


def draw_upwind_signs(key, part):
    line_key = jax.random.fold_in(key, 11)
    pulse_seed_handle = jax.random.fold_in(key, 12)
    other_key = jax.random.fold_in(key, 13)
    cross_key = jax.random.fold_in(key, 14)
    mesh_row_index = 2 * jax.random.randint(line_key, (1, SPAN_COUNT_DEPTH, SPAN_COUNT_HEIGHT), 0, 2) - 1
    stochastic_pulse = jax.random.randint(pulse_seed_handle, (SPAN_COUNT_WIDTH, SPAN_COUNT_DEPTH, SPAN_COUNT_HEIGHT), 0, 128) == 0
    remaining_piece = jax.random.randint(other_key, (SPAN_COUNT_WIDTH, SPAN_COUNT_DEPTH, SPAN_COUNT_HEIGHT), -1, 2)
    sweep_direction = jnp.where(stochastic_pulse, remaining_piece, jnp.broadcast_to(mesh_row_index, (SPAN_COUNT_WIDTH, SPAN_COUNT_DEPTH, SPAN_COUNT_HEIGHT)))
    across = jax.random.randint(cross_key, (2, SPAN_COUNT_WIDTH, SPAN_COUNT_DEPTH, SPAN_COUNT_HEIGHT), -1, 2)
    return jnp.concatenate([sweep_direction[None], across], axis=0).astype(jnp.int32)


def draw_line_decay(key, part):
    first_key = jax.random.fold_in(key, 0)
    return jnp.exp(jax.random.uniform(first_key, (SPAN_COUNT_DEPTH, SPAN_COUNT_HEIGHT), jnp.float32, math.log(0.5 / SPAN_COUNT_WIDTH), math.log(1.0 / 16)))


def plant(values, own_key, smallest, largest):
    longest = values.shape.index(max(values.shape))
    spots = []
    for shift in (0, 1):
        where = [jax.random.randint(jax.random.fold_in(own_key, axis), (), 0, length) for axis, length in enumerate(values.shape)]
        where[longest] = (where[longest] + shift) % values.shape[longest]
        spots.append(tuple(where))
    return values.at[spots[0]].set(smallest).at[spots[1]].set(largest)


def level_of(key, dims, cuts, low, high):
    loudness, own = 1.0, jax.random.fold_in(key, 6)
    for position, shards_of in cuts:
        steps = jnp.exp(jax.random.uniform(jax.random.fold_in(own, position), (shards_of,), jnp.float32, low / len(cuts), high / len(cuts)))
        loudness = loudness * jnp.repeat(steps, dims[position] // shards_of).reshape([-1 if axis == position else 1 for axis in range(len(dims))])
    return loudness


def centred(stream_key, extent, scale, most, shards=(), held_as=jnp.bfloat16):
    gain = level_of(stream_key, extent, shards, -0.22, 0.18) if shards else 1.0
    values = jax.random.normal(stream_key, extent, jnp.float32) * scale * gain
    return jnp.minimum(jnp.maximum(values, -most), most).astype(held_as)


def setup_inputs(seed: int = 0, part: int = 0) -> dict:
    key_list = jax.random.split(jax.random.key(seed), 8)
    part_keys = jax.random.split(jax.random.fold_in(key_list[7], part), 8)
    forward_field = draw_forward_field(jax.random.fold_in(jax.random.fold_in(key_list[7], part), 71), part)
    adjoint_field = centred(part_keys[1], (6, SPAN_COUNT_WIDTH, SPAN_COUNT_DEPTH, SPAN_COUNT_HEIGHT), 1.0, 6.0, ((1, 16),), jnp.float32)
    level_set = centred(key_list[2], (SPAN_COUNT_WIDTH, SPAN_COUNT_DEPTH, SPAN_COUNT_HEIGHT), 1.5, 8.0, ((0, 16),), jnp.float32)
    region_labels = plant(jax.random.randint(key_list[3], (SPAN_COUNT_WIDTH, SPAN_COUNT_DEPTH, SPAN_COUNT_HEIGHT), 0, REGIONS), jax.random.fold_in(key_list[3], 1), 0, REGIONS - 1).astype(jnp.int32)
    upwind_signs = draw_upwind_signs(jax.random.fold_in(key_list[7], 71), part)
    contrast = jnp.clip(jax.random.uniform(part_keys[5], (REGIONS,), jnp.float32, -3.0, 3.0), -3.0, 3.0)
    line_decay = draw_line_decay(jax.random.fold_in(key_list[7], 71), part)
    return {"forward_field": forward_field, "adjoint_field": adjoint_field, "level_set": level_set, "region_labels": region_labels, "upwind_signs": upwind_signs, "contrast": contrast, "line_decay": line_decay}


weno_eps = 1e-06
redist_step = 0.3
move_step = 0.5
cross_step = 0.3
norm_floor = 0.5
half_log = math.log(1.5)
third_log = math.log(3.0)

def weno_blend(first, second, third, fourth, fifth):
    cand_one = first / 3.0 - 7.0 * second / 6.0 + 11.0 * third / 6.0
    cand_two = -second / 6.0 + 5.0 * third / 6.0 + fourth / 3.0
    cand_three = third / 3.0 + 5.0 * fourth / 6.0 - fifth / 6.0
    rough_one = 13.0 / 12.0 * (first - 2.0 * second + third) ** 2 + 0.25 * (first - 4.0 * second + 3.0 * third) ** 2
    rough_two = 13.0 / 12.0 * (second - 2.0 * third + fourth) ** 2 + 0.25 * (second - fourth) ** 2
    rough_three = 13.0 / 12.0 * (third - 2.0 * fourth + fifth) ** 2 + 0.25 * (3.0 * third - 4.0 * fourth + fifth) ** 2
    weight_one = 0.1 / (weno_eps + rough_one) ** 2
    weight_two = 0.6 / (weno_eps + rough_two) ** 2
    weight_three = 0.3 / (weno_eps + rough_three) ** 2
    return (weight_one * cand_one + weight_two * cand_two + weight_three * cand_three) / (weight_one + weight_two + weight_three)

def slab_sides(extended):
    slopes = extended[1:] - extended[:-1]
    length = extended.shape[0] - 6

    def shifted(offset):
        return slopes[offset:offset + length]
    minus = weno_blend(shifted(0), shifted(1), shifted(2), shifted(3), shifted(4))
    plus = weno_blend(shifted(5), shifted(4), shifted(3), shifted(2), shifted(1))
    return (minus, plus)

def roll_sides(field, axis):
    slopes = jnp.roll(field, -1, axis) - field

    def shifted(offset):
        return jnp.roll(slopes, offset, axis)
    minus = weno_blend(shifted(3), shifted(2), shifted(1), slopes, shifted(-1))
    plus = weno_blend(shifted(-2), shifted(-1), slopes, shifted(1), shifted(2))
    return (minus, plus)

def godunov(pairs, sign):
    total = jnp.zeros_like(sign)
    for minus, plus in pairs:
        rising = jnp.maximum(jnp.maximum(minus, 0.0) ** 2, jnp.minimum(plus, 0.0) ** 2)
        falling = jnp.maximum(jnp.minimum(minus, 0.0) ** 2, jnp.maximum(plus, 0.0) ** 2)
        total = total + jnp.where(sign >= 0, rising, falling)
    return jnp.sqrt(total + 1e-12)

def gradient_size(extended, sign):
    core = extended[3:-3]
    return godunov((slab_sides(extended), roll_sides(core, 1), roll_sides(core, 2)), sign)

def unit_normal(extended, width):
    length = extended.shape[0] - 2 * width
    core = extended[width:width + length]
    grad_x = 0.5 * (extended[width + 1:width + 1 + length] - extended[width - 1:width - 1 + length])
    grad_y = 0.5 * (jnp.roll(core, -1, 1) - jnp.roll(core, 1, 1))
    grad_z = 0.5 * (jnp.roll(core, -1, 2) - jnp.roll(core, 1, 2))
    size = jnp.maximum(jnp.sqrt(grad_x * grad_x + grad_y * grad_y + grad_z * grad_z), norm_floor)
    return (grad_x / size, grad_y / size, grad_z / size)

def redistance(extended, sign):
    core = extended[3:-3]
    return core - redist_step * sign * (gradient_size(extended, sign) - 1.0)

def rates(decay, normal_x, signs):
    base = decay[None] * (0.5 + normal_x * normal_x)
    ahead = base + jnp.where(signs > 0, 0.0, jnp.where(signs == 0, half_log, third_log))
    back = base + jnp.where(signs < 0, 0.0, jnp.where(signs == 0, half_log, third_log))
    return (ahead, back)

def coefficients(rate, speed):
    return (jnp.exp(-rate), jnp.sqrt(-jnp.expm1(-2.0 * rate)) * speed)

def cross_update(speed, normal_y, normal_z, sign_y, sign_z):
    along_y = jnp.where(sign_y > 0, speed - jnp.roll(speed, 1, 1), jnp.where(sign_y < 0, speed - jnp.roll(speed, -1, 1), 0.0))
    along_z = jnp.where(sign_z > 0, speed - jnp.roll(speed, 1, 2), jnp.where(sign_z < 0, speed - jnp.roll(speed, -1, 2), 0.0))
    return speed - cross_step * (jnp.abs(normal_y) * along_y + jnp.abs(normal_z) * along_z)

def sweep(rate, speed, reverse):
    keep, push = coefficients(rate, speed)

    def advance(state, item):
        state = item[0] * state + item[1]
        return (state, state)
    start = jnp.zeros(keep.shape[1:], jnp.float32)
    _, result = lax.scan(advance, start, (keep, push), reverse=reverse)
    return result

def pad_slab(field):
    return jnp.pad(field, ((3, 3), (0, 0), (0, 0)))

def reference(forward_field, adjoint_field, level_set, region_labels, upwind_signs, contrast, line_decay):
    coupling = lax.optimization_barrier(jnp.sum(forward_field * adjoint_field, axis=0))
    material = jnp.zeros(level_set.shape, jnp.float32)
    for region in range(REGIONS):
        material = material + jnp.where(region_labels == region, contrast[region], 0.0)
    raw_speed = material * coupling
    power = jnp.sum(raw_speed * raw_speed) / (SPAN_COUNT_WIDTH * SPAN_COUNT_DEPTH * SPAN_COUNT_HEIGHT)
    speed = raw_speed / jnp.sqrt(power + 1e-06)
    sign_start = level_set / jnp.sqrt(level_set * level_set + 1.0)
    level = level_set
    for step in range(ITERS):
        extended = pad_slab(level)
        normal_x, normal_y, normal_z = unit_normal(extended, 3)
        ahead, back = rates(line_decay, normal_x, upwind_signs[0])
        speed = sweep(ahead, speed, False)
        speed = sweep(back, speed, True)
        speed = cross_update(speed, normal_y, normal_z, upwind_signs[1], upwind_signs[2])
        level = redistance(extended, sign_start)
    extended = pad_slab(level)
    moved = level - move_step * speed * gradient_size(extended, speed)
    return (moved, speed)
```

```python
import functools

import jax
import jax.numpy as jnp
from jax import lax
from jax.experimental import pallas as pl
from jax.experimental.pallas import tpu as pltpu
from jax.sharding import PartitionSpec as P

ITERS = 2
OWNERS = 4
MESH = pl.DeviceIdType.MESH

weno_eps = 1e-06
redist_step = 0.3
move_step = 0.5
cross_step = 0.3


def shift(a, step, axis):
    return pltpu.roll(a, (-step) % a.shape[axis], axis)


def weno_pair(d0, e0, e1, qm, q0, qp):
    c = 13.0 / 12.0
    hm, hp = 0.5 * qm, 0.5 * qp
    r1, r2, r3 = e0 + hm, 0.5 * (e0 + e1), e1 - hp
    s1 = c * qm * qm + (r1 * r1 + weno_eps)
    s2 = c * q0 * q0 + (r2 * r2 + weno_eps)
    s3 = c * qp * qp + (r3 * r3 + weno_eps)
    t1, t2, t3 = s1 * s1, s2 * s2, s3 * s3
    m1, m2, m3 = t2 * t3, t1 * t3, t1 * t2
    six = 6.0 * m2
    den_minus = m1 + six + 3.0 * m3
    den_plus = m3 + six + 3.0 * m1
    common = (2.0 * q0) * m2
    top = 1.5 * q0
    num_minus = common + m1 * (qm * (1.0 / 3.0)) + m3 * (top - hp)
    num_plus = common + m3 * (qp * (1.0 / 3.0)) + m1 * (top - hm)
    return (d0 + 0.5 * e0 + num_minus / den_minus, d0 - 0.5 * e1 + num_plus / den_plus)


def rolled_sides(f, axis):
    d0 = shift(f, 1, axis) - f
    e0 = d0 - shift(d0, -1, axis)
    e1 = shift(e0, 1, axis)
    q0 = e1 - e0
    following, plus = weno_pair(d0, e0, e1, shift(q0, -1, axis), q0, shift(q0, 1, axis))
    return shift(following, -1, axis), plus


def slab_center(ext, e, c):
    f = [ext[e, c + k] for k in range(-2, 4)]
    d = [b - a for a, b in zip(f, f[1:])]
    s = [b - a for a, b in zip(d, d[1:])]
    q = [b - a for a, b in zip(s, s[1:])]
    return weno_pair(d[2], s[1], s[2], q[0], q[1], q[2])


def loop_slab(length, ext, e, body):
    first, _ = slab_center(ext, e, 2)

    def one(i, minus_x):
        following, plus_x = slab_center(ext, e, i + 3)
        core = ext[e, i + 3]
        body(i, ((minus_x, plus_x), rolled_sides(core, 0), rolled_sides(core, 1)))
        return following

    lax.fori_loop(0, length, one, first)


def kernel(
    n, base,
    fwd_hbm, adj_hbm, lvl_hbm, lab_hbm, sgn_hbm, contrast, decay,
    moved_out, speed_out,
    fwd, adj, lab, sgn, ext, speed, kf, pf, kb, pb, kfc, cross, gain, kbc, u0, g_up, g_down,
    snd_c, snd_s, in_c, in_s, out_b, resp, pow_s, pow_in, pow_out, pow_res,
    load_sem, halo_send, halo_recv, c_send, c_recv, s_send, s_recv, r_send, r_recv,
    p_send, p_recv, q_send, q_recv,
):
    me = lax.axis_index("gx")
    corner = lax.axis_index("corner")
    length = lvl_hbm.shape[0]
    rows = lvl_hbm.shape[1] // OWNERS
    owner_no = (me - base) // 2
    is_owner = (me >= base) & (me < base + 2 * OWNERS) & (lax.rem(me - base + 2 * n, 2) == 0)

    def each(body):
        if n <= 16:
            for p in range(n):
                body(p)
        else:
            lax.fori_loop(0, n, lambda p, c: (body(p), c)[1], 0)

    loads = [
        pltpu.make_async_copy(src, dst, load_sem.at[k])
        for k, (src, dst) in enumerate((
            (lvl_hbm, ext.at[0, pl.ds(3, length)]), (fwd_hbm, fwd), (adj_hbm, adj),
            (lab_hbm, lab), (sgn_hbm, sgn)))
    ]
    for copy in loads:
        copy.start()

    barrier = pltpu.get_barrier_semaphore()

    def greet(p):
        @pl.when(p != me)
        def _():
            pl.semaphore_signal(barrier, inc=1, device_id=(corner, p), device_id_type=MESH)

    each(greet)

    @pl.when(me == 0)
    def _():
        for e in range(ITERS + 1):
            ext[e, 0:3] = jnp.zeros((3,) + ext.shape[2:], jnp.float32)

    @pl.when(me == n - 1)
    def _():
        for e in range(ITERS + 1):
            ext[e, length + 3 : length + 6] = jnp.zeros((3,) + ext.shape[2:], jnp.float32)

    loads[0].wait()
    pl.semaphore_wait(barrier, n - 1)

    def halo_copy(e, side, part):
        planes = 1 if part == 0 else 2
        if side == 0:
            src, dst = (length + 2, 2) if part == 0 else (length, 0)
        else:
            src, dst = (3, length + 3) if part == 0 else (4, length + 4)
        return pltpu.make_async_remote_copy(
            src_ref=ext.at[e, pl.ds(src, planes)],
            dst_ref=ext.at[e, pl.ds(dst, planes)],
            send_sem=halo_send.at[e, side, part],
            recv_sem=halo_recv.at[e, side, part],
            device_id=(corner, me + 1 if side == 0 else me - 1),
            device_id_type=MESH,
        )

    def halo_start(e):
        for part in range(2):
            for side in range(2):
                @pl.when((me < n - 1) if side == 0 else (me > 0))
                def _():
                    halo_copy(e, side, part).start()

    def halo_wait(e, part):
        for side in range(2):
            @pl.when((me > 0) if side == 0 else (me < n - 1))
            def _():
                halo_copy(e, side, part).wait_recv()

    halo_start(0)

    def to_owner(it, k, snd, dst, send, recv):
        owner = base + 2 * k
        src = snd.at[it, :, pl.ds(k * rows, rows), :]
        remote = pltpu.make_async_remote_copy(
            src_ref=src, dst_ref=dst.at[it, me], send_sem=send.at[it, k], recv_sem=recv.at[it],
            device_id=(corner, owner), device_id_type=MESH,
        )
        return owner, remote, pltpu.make_async_copy(src, dst.at[it, me], recv.at[it])

    def phase_one(it, snd, dst, send, recv):
        for k in range(OWNERS):
            owner, remote, local = to_owner(it, k, snd, dst, send, recv)

            @pl.when(me != owner)
            def _():
                remote.start()

            @pl.when(me == owner)
            def _():
                local.start()

    for copy in loads[1:4]:
        copy.wait()
    regions = contrast.shape[0]

    def raw(i, acc):
        coupling = fwd[0, i] * adj[0, i]
        for k in range(1, fwd.shape[0]):
            coupling = coupling + fwd[k, i] * adj[k, i]
        labels = lab[i]
        material = jnp.zeros(labels.shape, jnp.float32)
        for region in range(regions):
            material = jnp.where(labels == region, contrast[region], material)
        value = material * coupling
        speed[i] = value
        return acc + value * value

    squares = lax.fori_loop(0, length, raw, jnp.zeros(decay.shape, jnp.float32))
    tile = squares[0:8]
    for k in range(8, squares.shape[0], 8):
        tile = tile + squares[k : k + 8]
    pow_s[...] = tile

    def pow_copy():
        return pltpu.make_async_remote_copy(
            src_ref=pow_s, dst_ref=pow_in.at[me], send_sem=p_send.at[0], recv_sem=p_recv.at[0],
            device_id=(corner, base), device_id_type=MESH,
        )

    @pl.when(me != base)
    def _():
        pow_copy().start()

    @pl.when(me == base)
    def _():
        pltpu.make_async_copy(pow_s, pow_in.at[me], p_recv.at[0]).start()

    loads[4].wait()

    def coefficients(it):
        halo_wait(it, 0)

        def one(i, carry):
            f = ext[it, i + 3]
            gx = 0.5 * (ext[it, i + 4] - ext[it, i + 2])
            gy = 0.5 * (shift(f, 1, 0) - shift(f, -1, 0))
            gz = 0.5 * (shift(f, 1, 1) - shift(f, -1, 1))
            inv = lax.rsqrt(jnp.maximum(gx * gx + gy * gy + gz * gz, 0.25))
            nx = gx * inv
            y = decay[...] * (0.5 + nx * nx)
            t = y * (1.0 - y * 0.5 * (1.0 - y * (1.0 / 3.0) * (1.0 - y * 0.25 * (1.0 - y * 0.2))))
            keep = 1.0 - t
            z = t * (2.0 - t)
            sx = sgn[0, i]
            third = jnp.float32(1.0 / 3.0)
            two = jnp.float32(2.0 / 3.0)
            one_ = jnp.float32(1.0)
            mf = jnp.where(sx > 0, one_, jnp.where(sx == 0, two, third))
            mb = jnp.where(sx < 0, one_, jnp.where(sx == 0, two, third))
            a9, a4 = jnp.float32(1.0 / 9.0), jnp.float32(4.0 / 9.0)
            vf = jnp.where(sx > 0, one_, jnp.where(sx == 0, a4, a9))
            vb = jnp.where(sx < 0, one_, jnp.where(sx == 0, a4, a9))
            kf[i] = keep * mf
            kb[i] = keep * mb
            pf[i] = jnp.sqrt((1.0 - vf) + vf * z)
            pb[i] = jnp.sqrt((1.0 - vb) + vb * z)
            cross[it, 0, i] = cross_step * jnp.abs(gy * inv) * sgn[1, i].astype(jnp.float32)
            cross[it, 1, i] = cross_step * jnp.abs(gz * inv) * sgn[2, i].astype(jnp.float32)
            return carry

        lax.fori_loop(0, length, one, 0)
        run = kf[0]
        kfc[0] = run
        for i in range(1, length):
            run = run * kf[i]
            kfc[i] = run
        snd_c[it, 0] = run
        g, k = pb[length - 1] * kfc[length - 1], kb[length - 1]
        gain[it, length - 1] = g
        kbc[it, length - 1] = k
        for i in range(length - 2, -1, -1):
            g = kb[i] * g + pb[i] * kfc[i]
            k = k * kb[i]
            gain[it, i] = g
            kbc[it, i] = k
        snd_c[it, 1] = k
        snd_c[it, 2] = g
        phase_one(it, snd_c, in_c, c_send, c_recv)

    def sweeps(it):
        w = pf[0] * speed[0]
        speed[0] = w
        for i in range(1, length):
            w = kf[i] * w + pf[i] * speed[i]
            speed[i] = w
        snd_s[it, 0] = w
        u = pb[length - 1] * w
        u0[length - 1] = u
        for i in range(length - 2, -1, -1):
            u = kb[i] * u + pb[i] * speed[i]
            u0[i] = u
        snd_s[it, 1] = u
        phase_one(it, snd_s, in_s, s_send, s_recv)

    def redistance(e):
        halo_wait(e, 1)

        def body(i, pairs):
            start = ext[0, i + 3]
            up = start >= 0.0
            total = jnp.full(start.shape, 1e-12, jnp.float32)
            for minus, plus in pairs:
                other = -plus
                v = jnp.where(up, jnp.maximum(minus, other), -jnp.minimum(minus, other))
                v = jnp.maximum(v, 0.0)
                total = total + v * v
            sign = start * lax.rsqrt(start * start + 1.0)
            ext[e + 1, i + 3] = ext[e, i + 3] - redist_step * sign * (jnp.sqrt(total) - 1.0)

        loop_slab(length, ext, e, body)
        halo_start(e + 1)

    def both_sizes(e):
        halo_wait(e, 0)
        halo_wait(e, 1)

        def body(i, pairs):
            rise = jnp.full(g_up.shape[1:], 1e-12, jnp.float32)
            fall = rise
            for minus, plus in pairs:
                other = -plus
                hi = jnp.maximum(jnp.maximum(minus, other), 0.0)
                lo = jnp.minimum(jnp.minimum(minus, other), 0.0)
                rise = rise + hi * hi
                fall = fall + lo * lo
            g_up[i] = jnp.sqrt(rise)
            g_down[i] = jnp.sqrt(fall)

        loop_slab(length, ext, e, body)

    def reply(it, p):
        src = out_b.at[it, p]
        dst = resp.at[it, :, pl.ds(pl.multiple_of(owner_no * rows, rows), rows), :]
        remote = pltpu.make_async_remote_copy(
            src_ref=src, dst_ref=dst, send_sem=r_send.at[it, p], recv_sem=r_recv.at[it],
            device_id=(corner, p), device_id_type=MESH,
        )
        return remote, pltpu.make_async_copy(src, dst, r_recv.at[it])

    def own(it):
        @pl.when(is_owner)
        def _():
            pltpu.make_async_copy(in_c.at[it], in_c.at[it], c_recv.at[it]).wait()
            pltpu.make_async_copy(in_s.at[it], in_s.at[it], s_recv.at[it]).wait()
            zero = jnp.zeros(in_s.shape[3:], jnp.float32)

            def ahead(p, w):
                out_b[it, p, 0] = w
                return in_c[it, p, 0] * w + in_s[it, p, 0]

            def back(turn, u):
                p = n - 1 - turn
                out_b[it, p, 1] = u
                return in_c[it, p, 1] * u + (in_c[it, p, 2] * out_b[it, p, 0] + in_s[it, p, 1])

            lax.fori_loop(0, n, ahead, zero, unroll=n <= 16)
            lax.fori_loop(0, n, back, zero, unroll=n <= 16)

            def send(p):
                remote, local = reply(it, p)

                @pl.when(p != me)
                def _():
                    remote.start()

                @pl.when(p == me)
                def _():
                    local.start()

            each(send)

    def pow_reply(p):
        remote = pltpu.make_async_remote_copy(
            src_ref=pow_out, dst_ref=pow_res, send_sem=q_send.at[p], recv_sem=q_recv.at[0],
            device_id=(corner, p), device_id_type=MESH,
        )
        return remote, pltpu.make_async_copy(pow_out, pow_res, q_recv.at[0])

    def own_power():
        @pl.when(me == base)
        def _():
            pltpu.make_async_copy(pow_in, pow_in, p_recv.at[0]).wait()
            pow_out[...] = lax.fori_loop(
                0, n, lambda p, acc: acc + pow_in[p], jnp.zeros(pow_out.shape, jnp.float32)
            )

            def send(p):
                remote, local = pow_reply(p)

                @pl.when(p != me)
                def _():
                    remote.start()

                @pl.when(p == me)
                def _():
                    local.start()

            each(send)

    def finish(it, body):
        pltpu.make_async_copy(resp.at[it], resp.at[it], r_recv.at[it]).wait()

        def one(i, carry):
            s = u0[i] + gain[it, i] * resp[it, 0] + kbc[it, i] * resp[it, 1]
            cy, cz = cross[it, 0, i], cross[it, 1, i]
            near_y = jnp.where(cy > 0.0, shift(s, -1, 0), shift(s, 1, 0))
            near_z = jnp.where(cz > 0.0, shift(s, -1, 1), shift(s, 1, 1))
            body(i, s - (jnp.abs(cy) * (s - near_y) + jnp.abs(cz) * (s - near_z)))
            return carry

        lax.fori_loop(0, length, one, 0)

    def keep_speed(i, s):
        speed[i] = s

    coefficients(0)
    sweeps(0)
    for it in range(ITERS):
        last = it == ITERS - 1
        if not last:
            redistance(it)
            own(it)
            if it == 0:
                own_power()
            coefficients(it + 1)
            if it + 1 == ITERS - 1:
                redistance(it + 1)
            finish(it, keep_speed)
            sweeps(it + 1)
        else:
            both_sizes(it + 1)
            own(it)

    pltpu.make_async_copy(pow_res, pow_res, q_recv.at[0]).wait()
    cells = length * decay.shape[0] * decay.shape[1] * n
    total = jnp.sum(pow_res[...], keepdims=True)
    scale = lax.rsqrt(total * (1.0 / cells) + 1e-06)

    def emit(i, s):
        s = s * scale
        speed_out[i] = s
        size = jnp.where(s >= 0.0, g_up[i], g_down[i])
        moved_out[i] = ext[ITERS, i + 3] - move_step * s * size

    finish(ITERS - 1, emit)

    for e in range(ITERS + 1):
        for part in range(2):
            for side in range(2):
                @pl.when((me < n - 1) if side == 0 else (me > 0))
                def _():
                    halo_copy(e, side, part).wait_send()

    for it in range(ITERS):
        for k in range(OWNERS):
            for args in ((snd_c, in_c, c_send, c_recv), (snd_s, in_s, s_send, s_recv)):
                owner, remote, _ = to_owner(it, k, *args)

                @pl.when(me != owner)
                def _():
                    remote.wait_send()

    @pl.when(me != base)
    def _():
        pow_copy().wait_send()

    @pl.when(is_owner)
    def _():
        for it in range(ITERS):
            def done(p):
                @pl.when(p != me)
                def _():
                    reply(it, p)[0].wait_send()

            each(done)

    @pl.when(me == base)
    def _():
        def done(p):
            @pl.when(p != me)
            def _():
                pow_reply(p)[0].wait_send()

        each(done)


def solution(mesh):
    n = mesh.shape["gx"]
    base = n // 2 - OWNERS

    def shards(forward, adjoint, level, labels, signs, contrast, decay):
        slab = level.shape
        length, depth, height = slab
        rows = depth // OWNERS
        f32 = jnp.float32
        vm = lambda *shape: pltpu.VMEM(shape, f32)
        sems = lambda *shape: pltpu.SemaphoreType.DMA(shape)
        any_ = pl.BlockSpec(memory_space=pl.ANY)
        vmem = pl.BlockSpec(memory_space=pltpu.VMEM)
        return pl.pallas_call(
            functools.partial(kernel, n, base),
            out_shape=(jax.ShapeDtypeStruct(slab, f32), jax.ShapeDtypeStruct(slab, f32)),
            in_specs=[any_] * 5 + [pl.BlockSpec(memory_space=pltpu.SMEM), vmem],
            out_specs=(vmem, vmem),
            scratch_shapes=[
                vm(*forward.shape), vm(*adjoint.shape),
                pltpu.VMEM(slab, jnp.int32), pltpu.VMEM(signs.shape, jnp.int32),
                vm(ITERS + 1, length + 6, depth, height),
                vm(*slab), vm(*slab), vm(*slab), vm(*slab), vm(*slab), vm(*slab),
                vm(ITERS, 2, *slab), vm(ITERS, *slab), vm(ITERS, *slab), vm(*slab),
                vm(*slab), vm(*slab),
                vm(ITERS, 3, depth, height), vm(ITERS, 2, depth, height),
                vm(ITERS, n, 3, rows, height), vm(ITERS, n, 2, rows, height),
                vm(ITERS, n, 2, rows, height), vm(ITERS, 2, depth, height),
                vm(8, height), vm(n, 8, height), vm(8, height), vm(8, height),
                sems(5), sems(ITERS + 1, 2, 2), sems(ITERS + 1, 2, 2),
                sems(ITERS, OWNERS), sems(ITERS), sems(ITERS, OWNERS), sems(ITERS),
                sems(ITERS, n), sems(ITERS), sems(1), sems(1), sems(n), sems(1),
            ],
            compiler_params=pltpu.CompilerParams(collective_id=0, has_side_effects=True),
        )(forward, adjoint, level, labels, signs, contrast, decay)

    return jax.shard_map(
        shards,
        mesh=mesh,
        in_specs=(
            P(None, ("corner", "gx"), None, None),
            P(None, ("corner", "gx"), None, None),
            P("gx", None, None),
            P("gx", None, None),
            P(None, "gx", None, None),
            P("corner"),
            P(),
        ),
        out_specs=(P(("corner", "gx"), None, None), P(("corner", "gx"), None, None)),
        check_vma=False,
    )
```

```python
import functools

import jax
import jax.numpy as jnp
from jax import lax
from jax.experimental import pallas as pl
from jax.experimental.pallas import tpu as pltpu
from jax.sharding import PartitionSpec as P

ITERS = 2
OWNERS = 4
MESH = pl.DeviceIdType.MESH

weno_eps = 1e-06
redist_step = 0.3
move_step = 0.5
cross_step = 0.3


def shift(a, step, axis):
    return pltpu.roll(a, (-step) % a.shape[axis], axis)


def weno_pair(d0, e0, e1, qm, q0, qp):
    c = 13.0 / 3.0
    r1, r2, r3 = e0 + (e0 + qm), e0 + e1, e1 + (e1 - qp)
    s1 = c * qm * qm + (r1 * r1 + 4.0 * weno_eps)
    s2 = c * q0 * q0 + (r2 * r2 + 4.0 * weno_eps)
    s3 = c * qp * qp + (r3 * r3 + 4.0 * weno_eps)
    t1, t2, t3 = s1 * s1, s2 * s2, s3 * s3
    m1, m2, m3 = t2 * t3, t1 * t3, t1 * t2
    six, three_1, three_3 = 6.0 * m2, 3.0 * m1, 3.0 * m3
    common = six * q0
    top = 1.5 * q0
    num_minus = m1 * qm + common + three_3 * (top - 0.5 * qp)
    num_plus = m3 * qp + common + three_1 * (top - 0.5 * qm)
    d3 = 3.0 * d0
    return (
        d3 + 1.5 * e0 + num_minus / (m1 + six + three_3),
        d3 - 1.5 * e1 + num_plus / (m3 + six + three_1),
    )


def rolled_sides(f, axis):
    d0 = shift(f, 1, axis) - f
    e0 = d0 - shift(d0, -1, axis)
    e1 = shift(e0, 1, axis)
    q0 = e1 - e0
    following, plus = weno_pair(d0, e0, e1, shift(q0, -1, axis), q0, shift(q0, 1, axis))
    return shift(following, -1, axis), plus


def slab_pass(length, ext, e, body):
    for r in range(0, ext.shape[2], 8):
        at = slice(r, r + 8)
        f = [ext[e, c, at] for c in range(length + 6)]
        d = [b - a for a, b in zip(f, f[1:])]
        s = [b - a for a, b in zip(d, d[1:])]
        q = [b - a for a, b in zip(s, s[1:])]
        minus = None
        for c in range(2, length + 3):
            following, plus = weno_pair(d[c], s[c - 1], s[c], q[c - 2], q[c - 1], q[c])
            if c > 2:
                body(c - 3, at, minus, plus)
            minus = following


def planes(length, body, unroll):
    if unroll == length:
        for i in range(length):
            body(i)
    else:
        def some(j, carry):
            for k in range(unroll):
                body(j * unroll + k)
            return carry

        lax.fori_loop(0, length // unroll, some, 0)


def kernel(
    n, base,
    fwd_hbm, adj_hbm, lvl_hbm, lab_hbm, sgn_hbm, contrast_hbm, decay_hbm,
    moved_hbm, speed_hbm,
    contrast, decay, moved_out, speed_out, base_size,
    fwd, adj, lab, sgn, ext, speed, kf, pf, kb, pb, kfc, cross, gain, kbc, u0, g_up, g_down,
    snd_c, snd_s, in_c, in_s, out_b, resp, pow_s, pow_in, pow_out, pow_res,
    load_sem, halo_send, halo_recv, c_send, c_recv, s_send, s_recv, r_send, r_recv,
    p_send, p_recv, q_send, q_recv, out_sem,
):
    me = lax.axis_index("gx")
    corner = lax.axis_index("corner")
    length = lvl_hbm.shape[0]
    rows = lvl_hbm.shape[1] // OWNERS
    owner_no = (me - base) // 2
    is_owner = (me >= base) & (me < base + 2 * OWNERS) & (lax.rem(me - base + 2 * n, 2) == 0)

    def each(body):
        if n <= 16:
            for p in range(n):
                body(p)
        else:
            lax.fori_loop(0, n, lambda p, c: (body(p), c)[1], 0)

    loads = [
        pltpu.make_async_copy(src, dst, load_sem.at[k])
        for k, (src, dst) in enumerate((
            (lvl_hbm, ext.at[0, pl.ds(3, length)]), (sgn_hbm, sgn), (decay_hbm, decay),
            (contrast_hbm, contrast), (lab_hbm, lab), (fwd_hbm, fwd), (adj_hbm, adj)))
    ]
    for copy in loads:
        copy.start()

    barrier = pltpu.get_barrier_semaphore()

    def is_own(p):
        return (p >= base) & (p < base + 2 * OWNERS) & (lax.rem(p - base + 2 * n, 2) == 0)

    def greet(p):
        p = jnp.int32(p)
        meets = is_owner | is_own(p) | (p == me - 1) | (p == me + 1)

        @pl.when((p != me) & meets)
        def _():
            pl.semaphore_signal(barrier, inc=1, device_id=(corner, p), device_id_type=MESH)

    each(greet)

    @pl.when(me == 0)
    def _():
        for e in range(ITERS + 1):
            ext[e, 0:3] = jnp.zeros((3,) + ext.shape[2:], jnp.float32)

    @pl.when(me == n - 1)
    def _():
        for e in range(ITERS + 1):
            ext[e, length + 3 : length + 6] = jnp.zeros((3,) + ext.shape[2:], jnp.float32)

    def beside(p, inside):
        return (inside & jnp.logical_not(is_own(p))).astype(jnp.int32)

    met = jnp.where(is_owner, n - 1, OWNERS + beside(me - 1, me > 0) + beside(me + 1, me < n - 1))

    def halo_copy(e, side, part):
        planes = 1 if part == 0 else 2
        if side == 0:
            src, dst = (length + 2, 2) if part == 0 else (length, 0)
        else:
            src, dst = (3, length + 3) if part == 0 else (4, length + 4)
        return pltpu.make_async_remote_copy(
            src_ref=ext.at[e, pl.ds(src, planes)],
            dst_ref=ext.at[e, pl.ds(dst, planes)],
            send_sem=halo_send.at[e, side, part],
            recv_sem=halo_recv.at[e, side, part],
            device_id=(corner, me + 1 if side == 0 else me - 1),
            device_id_type=MESH,
        )

    def halo_start(e):
        for part in range(2):
            for side in range(2):
                @pl.when((me < n - 1) if side == 0 else (me > 0))
                def _():
                    halo_copy(e, side, part).start()

    def halo_wait(e, part):
        for side in range(2):
            @pl.when((me > 0) if side == 0 else (me < n - 1))
            def _():
                halo_copy(e, side, part).wait_recv()

    def to_owner(it, k, snd, dst, send, recv):
        owner = base + 2 * k
        src = snd.at[it, :, pl.ds(k * rows, rows), :]
        remote = pltpu.make_async_remote_copy(
            src_ref=src, dst_ref=dst.at[it, me], send_sem=send.at[it, k], recv_sem=recv.at[it],
            device_id=(corner, owner), device_id_type=MESH,
        )
        return owner, remote, pltpu.make_async_copy(src, dst.at[it, me], recv.at[it])

    def phase_one(it, snd, dst, send, recv):
        for k in range(OWNERS):
            owner, remote, local = to_owner(it, k, snd, dst, send, recv)

            @pl.when(me != owner)
            def _():
                remote.start()

            @pl.when(me == owner)
            def _():
                local.start()

    def pow_copy():
        return pltpu.make_async_remote_copy(
            src_ref=pow_s, dst_ref=pow_in.at[me], send_sem=p_send.at[0], recv_sem=p_recv.at[0],
            device_id=(corner, base), device_id_type=MESH,
        )

    def send_power():
        @pl.when(me != base)
        def _():
            pow_copy().start()

        @pl.when(me == base)
        def _():
            pltpu.make_async_copy(pow_s, pow_in.at[me], p_recv.at[0]).start()

    regions = contrast.shape[0]

    def raw_speed():
        acc = jnp.zeros(decay.shape, jnp.float32)
        for i in range(length):
            coupling = fwd[0, i] * adj[0, i]
            for k in range(1, fwd.shape[0]):
                coupling = coupling + fwd[k, i] * adj[k, i]
            labels = lab[i]
            material = jnp.zeros(labels.shape, jnp.float32)
            for region in range(regions):
                material = jnp.where(labels == region, contrast[region], material)
            value = material * coupling
            speed[i] = value
            acc = acc + value * value
        tile = acc[0:8]
        for k in range(8, acc.shape[0], 8):
            tile = tile + acc[k : k + 8]
        pow_s[...] = tile

    def plane_rates(it, which):
        for i in which:
            f = ext[it, i + 3]
            gx = 0.5 * (ext[it, i + 4] - ext[it, i + 2])
            gy = 0.5 * (shift(f, 1, 0) - shift(f, -1, 0))
            gz = 0.5 * (shift(f, 1, 1) - shift(f, -1, 1))
            inv = lax.rsqrt(jnp.maximum(gx * gx + gy * gy + gz * gz, 0.25))
            nx = gx * inv
            y = decay[...] * (0.5 + nx * nx)
            t = y * (1.0 - y * 0.5 * (1.0 - y * (1.0 / 3.0) * (1.0 - y * 0.25 * (1.0 - y * 0.2))))
            keep = 1.0 - t
            z = t * (2.0 - t)
            sx = sgn[0, i]
            third = jnp.float32(1.0 / 3.0)
            two = jnp.float32(2.0 / 3.0)
            one_ = jnp.float32(1.0)
            mf = jnp.where(sx > 0, one_, jnp.where(sx == 0, two, third))
            mb = jnp.where(sx < 0, one_, jnp.where(sx == 0, two, third))
            a9, a4 = jnp.float32(1.0 / 9.0), jnp.float32(4.0 / 9.0)
            vf = jnp.where(sx > 0, one_, jnp.where(sx == 0, a4, a9))
            vb = jnp.where(sx < 0, one_, jnp.where(sx == 0, a4, a9))
            kf[i] = keep * mf
            kb[i] = keep * mb
            pf[i] = jnp.sqrt((1.0 - vf) + vf * z)
            pb[i] = jnp.sqrt((1.0 - vb) + vb * z)
            cross[it, 0, i] = cross_step * jnp.abs(gy * inv) * sgn[1, i].astype(jnp.float32)
            cross[it, 1, i] = cross_step * jnp.abs(gz * inv) * sgn[2, i].astype(jnp.float32)

    def coefficients(it):
        halo_wait(it, 0)
        plane_rates(it, (0, length - 1))
        run = kf[0]
        kfc[0] = run
        for i in range(1, length):
            run = run * kf[i]
            kfc[i] = run
        snd_c[it, 0] = run
        g, k = pb[length - 1] * kfc[length - 1], kb[length - 1]
        gain[it, length - 1] = g
        kbc[it, length - 1] = k
        for i in range(length - 2, -1, -1):
            g = kb[i] * g + pb[i] * kfc[i]
            k = k * kb[i]
            gain[it, i] = g
            kbc[it, i] = k
        snd_c[it, 1] = k
        snd_c[it, 2] = g
        phase_one(it, snd_c, in_c, c_send, c_recv)

    def sweeps(it):
        w = pf[0] * speed[0]
        speed[0] = w
        for i in range(1, length):
            w = kf[i] * w + pf[i] * speed[i]
            speed[i] = w
        snd_s[it, 0] = w
        u = pb[length - 1] * w
        u0[length - 1] = u
        for i in range(length - 2, -1, -1):
            u = kb[i] * u + pb[i] * speed[i]
            u0[i] = u
        snd_s[it, 1] = u
        phase_one(it, snd_s, in_s, s_send, s_recv)

    def across(e):
        both = e == ITERS

        def body(i):
            f = ext[e, i + 3]
            pairs = (rolled_sides(f, 0), rolled_sides(f, 1))
            if both:
                rise = fall = None
                for minus, plus in pairs:
                    hi = jnp.maximum(jnp.maximum(minus, -plus), 0.0)
                    lo = jnp.minimum(jnp.minimum(minus, -plus), 0.0)
                    rise = hi * hi if rise is None else rise + hi * hi
                    fall = lo * lo if fall is None else fall + lo * lo
                g_up[i] = rise
                g_down[i] = fall
            else:
                up = ext[0, i + 3] >= 0.0
                total = None
                for minus, plus in pairs:
                    v = jnp.where(up, jnp.maximum(minus, -plus), jnp.maximum(-minus, plus))
                    v = jnp.maximum(v, 0.0)
                    total = v * v if total is None else total + v * v
                base_size[i] = total

        planes(length, body, 2)

    def along(e):
        both = e == ITERS
        if both:
            halo_wait(e, 0)
        halo_wait(e, 1)
        ninth = 1.0 / 9.0

        def body(i, at, minus, plus):
            if both:
                hi = jnp.maximum(jnp.maximum(minus, -plus), 0.0)
                lo = jnp.minimum(jnp.minimum(minus, -plus), 0.0)
                g_up[i, at] = jnp.sqrt((g_up[i, at] + hi * hi) * ninth + 1e-12)
                g_down[i, at] = jnp.sqrt((g_down[i, at] + lo * lo) * ninth + 1e-12)
            else:
                start = ext[0, i + 3, at]
                v = jnp.where(start >= 0.0, jnp.maximum(minus, -plus), jnp.maximum(-minus, plus))
                v = jnp.maximum(v, 0.0)
                size = jnp.sqrt((base_size[i, at] + v * v) * ninth + 1e-12)
                sign = start * lax.rsqrt(start * start + 1.0)
                ext[e + 1, i + 3, at] = ext[e, i + 3, at] - redist_step * sign * (size - 1.0)

        slab_pass(length, ext, e, body)
        if not both:
            halo_start(e + 1)

    def reply(it, p):
        src = out_b.at[it, p]
        dst = resp.at[it, :, pl.ds(pl.multiple_of(owner_no * rows, rows), rows), :]
        remote = pltpu.make_async_remote_copy(
            src_ref=src, dst_ref=dst, send_sem=r_send.at[it, p], recv_sem=r_recv.at[it],
            device_id=(corner, p), device_id_type=MESH,
        )
        return remote, pltpu.make_async_copy(src, dst, r_recv.at[it])

    def own(it):
        @pl.when(is_owner)
        def _():
            pltpu.make_async_copy(in_c.at[it], in_c.at[it], c_recv.at[it]).wait()
            pltpu.make_async_copy(in_s.at[it], in_s.at[it], s_recv.at[it]).wait()
            zero = jnp.zeros(in_s.shape[3:], jnp.float32)

            def ahead(p, w):
                out_b[it, p, 0] = w
                return in_c[it, p, 0] * w + in_s[it, p, 0]

            def back(turn, u):
                p = n - 1 - turn
                out_b[it, p, 1] = u
                return in_c[it, p, 1] * u + (in_c[it, p, 2] * out_b[it, p, 0] + in_s[it, p, 1])

            lax.fori_loop(0, n, ahead, zero, unroll=n <= 16)
            lax.fori_loop(0, n, back, zero, unroll=n <= 16)

            def send(p):
                remote, local = reply(it, p)

                @pl.when(p != me)
                def _():
                    remote.start()

                @pl.when(p == me)
                def _():
                    local.start()

            each(send)

    def pow_reply(p):
        remote = pltpu.make_async_remote_copy(
            src_ref=pow_out, dst_ref=pow_res, send_sem=q_send.at[p], recv_sem=q_recv.at[0],
            device_id=(corner, p), device_id_type=MESH,
        )
        return remote, pltpu.make_async_copy(pow_out, pow_res, q_recv.at[0])

    def own_power():
        @pl.when(me == base)
        def _():
            pltpu.make_async_copy(pow_in, pow_in, p_recv.at[0]).wait()
            pow_out[...] = lax.fori_loop(
                0, n, lambda p, acc: acc + pow_in[p], jnp.zeros(pow_out.shape, jnp.float32)
            )

            def send(p):
                remote, local = pow_reply(p)

                @pl.when(p != me)
                def _():
                    remote.start()

                @pl.when(p == me)
                def _():
                    local.start()

            each(send)

    def finish(it, body):
        pltpu.make_async_copy(resp.at[it], resp.at[it], r_recv.at[it]).wait()

        for i in range(length):
            s = u0[i] + gain[it, i] * resp[it, 0] + kbc[it, i] * resp[it, 1]
            cy, cz = cross[it, 0, i], cross[it, 1, i]
            near_y = jnp.where(cy > 0.0, shift(s, -1, 0), shift(s, 1, 0))
            near_z = jnp.where(cz > 0.0, shift(s, -1, 1), shift(s, 1, 1))
            body(i, s - (jnp.abs(cy) * (s - near_y) + jnp.abs(cz) * (s - near_z)))

    def keep_speed(i, s):
        speed[i] = s

    inner = range(1, length - 1)
    for copy in loads[:3]:
        copy.wait()
    plane_rates(0, inner)
    for copy in loads[3:]:
        copy.wait()
    raw_speed()
    pl.semaphore_wait(barrier, met)
    halo_start(0)
    across(0)
    coefficients(0)
    sweeps(0)
    send_power()
    along(0)
    plane_rates(1, inner)
    across(1)
    own(0)
    own_power()
    coefficients(1)
    along(1)
    across(2)
    finish(0, keep_speed)
    sweeps(1)
    along(2)
    own(1)

    pltpu.make_async_copy(pow_res, pow_res, q_recv.at[0]).wait()
    cells = length * decay.shape[0] * decay.shape[1] * n
    total = jnp.sum(pow_res[...], keepdims=True)
    scale = lax.rsqrt(total * (1.0 / cells) + 1e-06)

    outs = [
        (pltpu.make_async_copy(src.at[i], dst.at[i], out_sem.at[k, i]))
        for i in range(length)
        for k, (src, dst) in enumerate(((moved_out, moved_hbm), (speed_out, speed_hbm)))
    ]

    def emit(i, s):
        s = s * scale
        speed_out[i] = s
        size = jnp.where(s >= 0.0, g_up[i], g_down[i])
        moved_out[i] = ext[ITERS, i + 3] - move_step * s * size
        outs[2 * i].start()
        outs[2 * i + 1].start()

    finish(ITERS - 1, emit)
    for copy in outs:
        copy.wait()

    for e in range(ITERS + 1):
        for part in range(2):
            for side in range(2):
                @pl.when((me < n - 1) if side == 0 else (me > 0))
                def _():
                    halo_copy(e, side, part).wait_send()

    for it in range(ITERS):
        for k in range(OWNERS):
            for args in ((snd_c, in_c, c_send, c_recv), (snd_s, in_s, s_send, s_recv)):
                owner, remote, _ = to_owner(it, k, *args)

                @pl.when(me != owner)
                def _():
                    remote.wait_send()

    @pl.when(me != base)
    def _():
        pow_copy().wait_send()

    @pl.when(is_owner)
    def _():
        for it in range(ITERS):
            def done(p):
                @pl.when(p != me)
                def _():
                    reply(it, p)[0].wait_send()

            each(done)

    @pl.when(me == base)
    def _():
        def done(p):
            @pl.when(p != me)
            def _():
                pow_reply(p)[0].wait_send()

        each(done)


def solution(mesh):
    n = mesh.shape["gx"]
    base = n // 2 - OWNERS

    def shards(forward, adjoint, level, labels, signs, contrast, decay):
        slab = level.shape
        length, depth, height = slab
        rows = depth // OWNERS
        f32 = jnp.float32
        vm = lambda *shape: pltpu.VMEM(shape, f32)
        sems = lambda *shape: pltpu.SemaphoreType.DMA(shape)
        any_ = pl.BlockSpec(memory_space=pl.ANY)
        return pl.pallas_call(
            functools.partial(kernel, n, base),
            out_shape=(jax.ShapeDtypeStruct(slab, f32), jax.ShapeDtypeStruct(slab, f32)),
            in_specs=[any_] * 7,
            out_specs=(any_, any_),
            scratch_shapes=[
                pltpu.SMEM(contrast.shape, f32), vm(depth, height), vm(*slab), vm(*slab), vm(*slab),
                vm(*forward.shape), vm(*adjoint.shape),
                pltpu.VMEM(slab, jnp.int32), pltpu.VMEM(signs.shape, jnp.int32),
                vm(ITERS + 1, length + 6, depth, height),
                vm(*slab), vm(*slab), vm(*slab), vm(*slab), vm(*slab), vm(*slab),
                vm(ITERS, 2, *slab), vm(ITERS, *slab), vm(ITERS, *slab), vm(*slab),
                vm(*slab), vm(*slab),
                vm(ITERS, 3, depth, height), vm(ITERS, 2, depth, height),
                vm(ITERS, n, 3, rows, height), vm(ITERS, n, 2, rows, height),
                vm(ITERS, n, 2, rows, height), vm(ITERS, 2, depth, height),
                vm(8, height), vm(n, 8, height), vm(8, height), vm(8, height),
                sems(7), sems(ITERS + 1, 2, 2), sems(ITERS + 1, 2, 2),
                sems(ITERS, OWNERS), sems(ITERS), sems(ITERS, OWNERS), sems(ITERS),
                sems(ITERS, n), sems(ITERS), sems(1), sems(1), sems(n), sems(1),
                sems(2, length),
            ],
            compiler_params=pltpu.CompilerParams(collective_id=0, has_side_effects=True),
        )(forward, adjoint, level, labels, signs, contrast, decay)

    return jax.shard_map(
        shards,
        mesh=mesh,
        in_specs=(
            P(None, ("corner", "gx"), None, None),
            P(None, ("corner", "gx"), None, None),
            P("gx", None, None),
            P("gx", None, None),
            P(None, "gx", None, None),
            P("corner"),
            P(),
        ),
        out_specs=(P(("corner", "gx"), None, None), P(("corner", "gx"), None, None)),
        check_vma=False,
    )
```

```python
import functools

import jax
import jax.numpy as jnp
from jax import lax
from jax.experimental import pallas as pl
from jax.experimental.pallas import tpu as pltpu
from jax.sharding import PartitionSpec as P

ITERS = 2
OWNERS = 4
MESH = pl.DeviceIdType.MESH

weno_eps = 1e-06
redist_step = 0.3
move_step = 0.5
cross_step = 0.3


def shift(a, step, axis):
    return pltpu.roll(a, (-step) % a.shape[axis], axis)


def weno_pair(d0, e0, e1, qm, q0, qp):
    c = 13.0 / 3.0
    r1, r2, r3 = e0 + (e0 + qm), e0 + e1, e1 + (e1 - qp)
    s1 = c * qm * qm + (r1 * r1 + 4.0 * weno_eps)
    s2 = c * q0 * q0 + (r2 * r2 + 4.0 * weno_eps)
    s3 = c * qp * qp + (r3 * r3 + 4.0 * weno_eps)
    t1, t2, t3 = s1 * s1, s2 * s2, s3 * s3
    m1, m2, m3 = t2 * t3, t1 * t3, t1 * t2
    six, three_1, three_3 = 6.0 * m2, 3.0 * m1, 3.0 * m3
    common = six * q0
    top = 1.5 * q0
    num_minus = m1 * qm + common + three_3 * (top - 0.5 * qp)
    num_plus = m3 * qp + common + three_1 * (top - 0.5 * qm)
    d3 = 3.0 * d0
    return (
        d3 + 1.5 * e0 + num_minus / (m1 + six + three_3),
        d3 - 1.5 * e1 + num_plus / (m3 + six + three_1),
    )


def rolled_sides(f, axis):
    d0 = shift(f, 1, axis) - f
    e0 = d0 - shift(d0, -1, axis)
    e1 = shift(e0, 1, axis)
    q0 = e1 - e0
    following, plus = weno_pair(d0, e0, e1, shift(q0, -1, axis), q0, shift(q0, 1, axis))
    return shift(following, -1, axis), plus


def slab_pass(length, ext, e, body):
    for r in range(0, ext.shape[2], 8):
        at = slice(r, r + 8)
        f = [ext[e, c, at] for c in range(length + 6)]
        d = [b - a for a, b in zip(f, f[1:])]
        s = [b - a for a, b in zip(d, d[1:])]
        q = [b - a for a, b in zip(s, s[1:])]
        minus = None
        for c in range(2, length + 3):
            following, plus = weno_pair(d[c], s[c - 1], s[c], q[c - 2], q[c - 1], q[c])
            if c > 2:
                body(c - 3, at, minus, plus)
            minus = following


def planes(length, body, unroll):
    if unroll == length:
        for i in range(length):
            body(i)
    else:
        def some(j, carry):
            for k in range(unroll):
                body(j * unroll + k)
            return carry

        lax.fori_loop(0, length // unroll, some, 0)


def kernel(
    n, base,
    fwd_hbm, adj_hbm, lvl_hbm, lab_hbm, sgn_hbm, contrast_hbm, decay_hbm,
    moved_out, speed_out,
    contrast, decay, base_size,
    fwd, adj, lab, sgn, ext, speed, kf, pf, kb, pb, kfc, cross, gain, kbc, u0, g_up, g_down,
    snd_c, snd_s, in_c, in_s, out_b, resp, pow_s, pow_in, pow_out, pow_res,
    load_sem, halo_send, halo_recv, c_send, c_recv, s_send, s_recv, r_send, r_recv,
    p_send, p_recv, q_send, q_recv,
):
    me = lax.axis_index("gx")
    corner = lax.axis_index("corner")
    length = lvl_hbm.shape[0]
    rows = lvl_hbm.shape[1] // OWNERS
    owner_no = (me - base) // 2
    is_owner = (me >= base) & (me < base + 2 * OWNERS) & (lax.rem(me - base + 2 * n, 2) == 0)

    def each(body):
        if n <= 16:
            for p in range(n):
                body(p)
        else:
            lax.fori_loop(0, n, lambda p, c: (body(p), c)[1], 0)

    loads = [
        pltpu.make_async_copy(src, dst, load_sem.at[k])
        for k, (src, dst) in enumerate((
            (lvl_hbm, ext.at[0, pl.ds(3, length)]), (sgn_hbm, sgn), (decay_hbm, decay),
            (contrast_hbm, contrast), (lab_hbm, lab), (fwd_hbm, fwd), (adj_hbm, adj)))
    ]
    for copy in loads:
        copy.start()

    barrier = pltpu.get_barrier_semaphore()

    def is_own(p):
        return (p >= base) & (p < base + 2 * OWNERS) & (lax.rem(p - base + 2 * n, 2) == 0)

    def greet(p):
        p = jnp.int32(p)
        meets = is_owner | is_own(p) | (p == me - 1) | (p == me + 1)

        @pl.when((p != me) & meets)
        def _():
            pl.semaphore_signal(barrier, inc=1, device_id=(corner, p), device_id_type=MESH)

    each(greet)

    @pl.when(me == 0)
    def _():
        for e in range(ITERS + 1):
            ext[e, 0:3] = jnp.zeros((3,) + ext.shape[2:], jnp.float32)

    @pl.when(me == n - 1)
    def _():
        for e in range(ITERS + 1):
            ext[e, length + 3 : length + 6] = jnp.zeros((3,) + ext.shape[2:], jnp.float32)

    def beside(p, inside):
        return (inside & jnp.logical_not(is_own(p))).astype(jnp.int32)

    met = jnp.where(is_owner, n - 1, OWNERS + beside(me - 1, me > 0) + beside(me + 1, me < n - 1))

    def halo_copy(e, side, part):
        planes = 1 if part == 0 else 2
        if side == 0:
            src, dst = (length + 2, 2) if part == 0 else (length, 0)
        else:
            src, dst = (3, length + 3) if part == 0 else (4, length + 4)
        return pltpu.make_async_remote_copy(
            src_ref=ext.at[e, pl.ds(src, planes)],
            dst_ref=ext.at[e, pl.ds(dst, planes)],
            send_sem=halo_send.at[e, side, part],
            recv_sem=halo_recv.at[e, side, part],
            device_id=(corner, me + 1 if side == 0 else me - 1),
            device_id_type=MESH,
        )

    def halo_start(e):
        for part in range(2):
            for side in range(2):
                @pl.when((me < n - 1) if side == 0 else (me > 0))
                def _():
                    halo_copy(e, side, part).start()

    def halo_wait(e, part):
        for side in range(2):
            @pl.when((me > 0) if side == 0 else (me < n - 1))
            def _():
                halo_copy(e, side, part).wait_recv()

    def to_owner(it, k, snd, dst, send, recv):
        owner = base + 2 * k
        src = snd.at[it, :, pl.ds(k * rows, rows), :]
        remote = pltpu.make_async_remote_copy(
            src_ref=src, dst_ref=dst.at[it, me], send_sem=send.at[it, k], recv_sem=recv.at[it],
            device_id=(corner, owner), device_id_type=MESH,
        )
        return owner, remote, pltpu.make_async_copy(src, dst.at[it, me], recv.at[it])

    def phase_one(it, snd, dst, send, recv):
        for k in range(OWNERS):
            owner, remote, local = to_owner(it, k, snd, dst, send, recv)

            @pl.when(me != owner)
            def _():
                remote.start()

            @pl.when(me == owner)
            def _():
                local.start()

    def pow_copy():
        return pltpu.make_async_remote_copy(
            src_ref=pow_s, dst_ref=pow_in.at[me], send_sem=p_send.at[0], recv_sem=p_recv.at[0],
            device_id=(corner, base), device_id_type=MESH,
        )

    def send_power():
        @pl.when(me != base)
        def _():
            pow_copy().start()

        @pl.when(me == base)
        def _():
            pltpu.make_async_copy(pow_s, pow_in.at[me], p_recv.at[0]).start()

    regions = contrast.shape[0]

    def raw_speed():
        acc = jnp.zeros(decay.shape, jnp.float32)
        for i in range(length):
            coupling = fwd[0, i] * adj[0, i]
            for k in range(1, fwd.shape[0]):
                coupling = coupling + fwd[k, i] * adj[k, i]
            labels = lab[i]
            material = jnp.zeros(labels.shape, jnp.float32)
            for region in range(regions):
                material = jnp.where(labels == region, contrast[region], material)
            value = material * coupling
            speed[i] = value
            acc = acc + value * value
        tile = acc[0:8]
        for k in range(8, acc.shape[0], 8):
            tile = tile + acc[k : k + 8]
        pow_s[...] = tile

    def plane_rates(it, which):
        for i in which:
            f = ext[it, i + 3]
            gx = 0.5 * (ext[it, i + 4] - ext[it, i + 2])
            gy = 0.5 * (shift(f, 1, 0) - shift(f, -1, 0))
            gz = 0.5 * (shift(f, 1, 1) - shift(f, -1, 1))
            inv = lax.rsqrt(jnp.maximum(gx * gx + gy * gy + gz * gz, 0.25))
            nx = gx * inv
            y = decay[...] * (0.5 + nx * nx)
            t = y * (1.0 - y * 0.5 * (1.0 - y * (1.0 / 3.0) * (1.0 - y * 0.25 * (1.0 - y * 0.2))))
            keep = 1.0 - t
            z = t * (2.0 - t)
            sx = sgn[0, i]
            third = jnp.float32(1.0 / 3.0)
            two = jnp.float32(2.0 / 3.0)
            one_ = jnp.float32(1.0)
            mf = jnp.where(sx > 0, one_, jnp.where(sx == 0, two, third))
            mb = jnp.where(sx < 0, one_, jnp.where(sx == 0, two, third))
            a9, a4 = jnp.float32(1.0 / 9.0), jnp.float32(4.0 / 9.0)
            vf = jnp.where(sx > 0, one_, jnp.where(sx == 0, a4, a9))
            vb = jnp.where(sx < 0, one_, jnp.where(sx == 0, a4, a9))
            kf[i] = keep * mf
            kb[i] = keep * mb
            pf[i] = jnp.sqrt((1.0 - vf) + vf * z)
            pb[i] = jnp.sqrt((1.0 - vb) + vb * z)
            cross[it, 0, i] = cross_step * jnp.abs(gy * inv) * sgn[1, i].astype(jnp.float32)
            cross[it, 1, i] = cross_step * jnp.abs(gz * inv) * sgn[2, i].astype(jnp.float32)

    def coefficients(it):
        halo_wait(it, 0)
        plane_rates(it, (0, length - 1))
        run = kf[0]
        kfc[0] = run
        for i in range(1, length):
            run = run * kf[i]
            kfc[i] = run
        snd_c[it, 0] = run
        g, k = pb[length - 1] * kfc[length - 1], kb[length - 1]
        gain[it, length - 1] = g
        kbc[it, length - 1] = k
        for i in range(length - 2, -1, -1):
            g = kb[i] * g + pb[i] * kfc[i]
            k = k * kb[i]
            gain[it, i] = g
            kbc[it, i] = k
        snd_c[it, 1] = k
        snd_c[it, 2] = g
        phase_one(it, snd_c, in_c, c_send, c_recv)

    def sweeps(it):
        w = pf[0] * speed[0]
        speed[0] = w
        for i in range(1, length):
            w = kf[i] * w + pf[i] * speed[i]
            speed[i] = w
        snd_s[it, 0] = w
        u = pb[length - 1] * w
        u0[length - 1] = u
        for i in range(length - 2, -1, -1):
            u = kb[i] * u + pb[i] * speed[i]
            u0[i] = u
        snd_s[it, 1] = u
        phase_one(it, snd_s, in_s, s_send, s_recv)

    def across(e):
        both = e == ITERS

        def body(i):
            f = ext[e, i + 3]
            pairs = (rolled_sides(f, 0), rolled_sides(f, 1))
            if both:
                rise = fall = None
                for minus, plus in pairs:
                    hi = jnp.maximum(jnp.maximum(minus, -plus), 0.0)
                    lo = jnp.minimum(jnp.minimum(minus, -plus), 0.0)
                    rise = hi * hi if rise is None else rise + hi * hi
                    fall = lo * lo if fall is None else fall + lo * lo
                g_up[i] = rise
                g_down[i] = fall
            else:
                up = ext[0, i + 3] >= 0.0
                total = None
                for minus, plus in pairs:
                    v = jnp.where(up, jnp.maximum(minus, -plus), jnp.maximum(-minus, plus))
                    v = jnp.maximum(v, 0.0)
                    total = v * v if total is None else total + v * v
                base_size[i] = total

        planes(length, body, 2)

    def along(e):
        both = e == ITERS
        if both:
            halo_wait(e, 0)
        halo_wait(e, 1)
        ninth = 1.0 / 9.0

        def body(i, at, minus, plus):
            if both:
                hi = jnp.maximum(jnp.maximum(minus, -plus), 0.0)
                lo = jnp.minimum(jnp.minimum(minus, -plus), 0.0)
                g_up[i, at] = jnp.sqrt((g_up[i, at] + hi * hi) * ninth + 1e-12)
                g_down[i, at] = jnp.sqrt((g_down[i, at] + lo * lo) * ninth + 1e-12)
            else:
                start = ext[0, i + 3, at]
                v = jnp.where(start >= 0.0, jnp.maximum(minus, -plus), jnp.maximum(-minus, plus))
                v = jnp.maximum(v, 0.0)
                size = jnp.sqrt((base_size[i, at] + v * v) * ninth + 1e-12)
                sign = start * lax.rsqrt(start * start + 1.0)
                ext[e + 1, i + 3, at] = ext[e, i + 3, at] - redist_step * sign * (size - 1.0)

        slab_pass(length, ext, e, body)
        if not both:
            halo_start(e + 1)

    def reply(it, p):
        src = out_b.at[it, p]
        dst = resp.at[it, :, pl.ds(pl.multiple_of(owner_no * rows, rows), rows), :]
        remote = pltpu.make_async_remote_copy(
            src_ref=src, dst_ref=dst, send_sem=r_send.at[it, p], recv_sem=r_recv.at[it],
            device_id=(corner, p), device_id_type=MESH,
        )
        return remote, pltpu.make_async_copy(src, dst, r_recv.at[it])

    def own(it):
        @pl.when(is_owner)
        def _():
            pltpu.make_async_copy(in_c.at[it], in_c.at[it], c_recv.at[it]).wait()
            pltpu.make_async_copy(in_s.at[it], in_s.at[it], s_recv.at[it]).wait()
            zero = jnp.zeros(in_s.shape[3:], jnp.float32)

            def ahead(p, w):
                out_b[it, p, 0] = w
                return in_c[it, p, 0] * w + in_s[it, p, 0]

            def back(turn, u):
                p = n - 1 - turn
                out_b[it, p, 1] = u
                return in_c[it, p, 1] * u + (in_c[it, p, 2] * out_b[it, p, 0] + in_s[it, p, 1])

            lax.fori_loop(0, n, ahead, zero, unroll=n <= 16)
            lax.fori_loop(0, n, back, zero, unroll=n <= 16)

            def send(p):
                remote, local = reply(it, p)

                @pl.when(p != me)
                def _():
                    remote.start()

                @pl.when(p == me)
                def _():
                    local.start()

            each(send)

    def pow_reply(p):
        remote = pltpu.make_async_remote_copy(
            src_ref=pow_out, dst_ref=pow_res, send_sem=q_send.at[p], recv_sem=q_recv.at[0],
            device_id=(corner, p), device_id_type=MESH,
        )
        return remote, pltpu.make_async_copy(pow_out, pow_res, q_recv.at[0])

    def own_power():
        @pl.when(me == base)
        def _():
            pltpu.make_async_copy(pow_in, pow_in, p_recv.at[0]).wait()
            pow_out[...] = lax.fori_loop(
                0, n, lambda p, acc: acc + pow_in[p], jnp.zeros(pow_out.shape, jnp.float32)
            )

            def send(p):
                remote, local = pow_reply(p)

                @pl.when(p != me)
                def _():
                    remote.start()

                @pl.when(p == me)
                def _():
                    local.start()

            each(send)

    def finish(it, body):
        pltpu.make_async_copy(resp.at[it], resp.at[it], r_recv.at[it]).wait()

        for i in range(length):
            s = u0[i] + gain[it, i] * resp[it, 0] + kbc[it, i] * resp[it, 1]
            cy, cz = cross[it, 0, i], cross[it, 1, i]
            near_y = jnp.where(cy > 0.0, shift(s, -1, 0), shift(s, 1, 0))
            near_z = jnp.where(cz > 0.0, shift(s, -1, 1), shift(s, 1, 1))
            body(i, s - (jnp.abs(cy) * (s - near_y) + jnp.abs(cz) * (s - near_z)))

    def keep_speed(i, s):
        speed[i] = s

    inner = range(1, length - 1)
    for copy in loads[:3]:
        copy.wait()
    plane_rates(0, inner)
    for copy in loads[3:]:
        copy.wait()
    raw_speed()
    pl.semaphore_wait(barrier, met)
    halo_start(0)
    across(0)
    coefficients(0)
    sweeps(0)
    send_power()
    along(0)
    plane_rates(1, inner)
    across(1)
    own(0)
    own_power()
    coefficients(1)
    along(1)
    across(2)
    finish(0, keep_speed)
    sweeps(1)
    along(2)
    own(1)

    pltpu.make_async_copy(pow_res, pow_res, q_recv.at[0]).wait()
    cells = length * decay.shape[0] * decay.shape[1] * n
    total = jnp.sum(pow_res[...], keepdims=True)
    scale = lax.rsqrt(total * (1.0 / cells) + 1e-06)

    def emit(i, s):
        s = s * scale
        speed_out[i] = s
        size = jnp.where(s >= 0.0, g_up[i], g_down[i])
        moved_out[i] = ext[ITERS, i + 3] - move_step * s * size

    finish(ITERS - 1, emit)
    for e in range(ITERS + 1):
        for part in range(2):
            for side in range(2):
                @pl.when((me < n - 1) if side == 0 else (me > 0))
                def _():
                    halo_copy(e, side, part).wait_send()

    for it in range(ITERS):
        for k in range(OWNERS):
            for args in ((snd_c, in_c, c_send, c_recv), (snd_s, in_s, s_send, s_recv)):
                owner, remote, _ = to_owner(it, k, *args)

                @pl.when(me != owner)
                def _():
                    remote.wait_send()

    @pl.when(me != base)
    def _():
        pow_copy().wait_send()

    @pl.when(is_owner)
    def _():
        for it in range(ITERS):
            def done(p):
                @pl.when(p != me)
                def _():
                    reply(it, p)[0].wait_send()

            each(done)

    @pl.when(me == base)
    def _():
        def done(p):
            @pl.when(p != me)
            def _():
                pow_reply(p)[0].wait_send()

        each(done)


def solution(mesh):
    n = mesh.shape["gx"]
    base = n // 2 - OWNERS + 1

    def shards(forward, adjoint, level, labels, signs, contrast, decay):
        slab = level.shape
        length, depth, height = slab
        rows = depth // OWNERS
        f32 = jnp.float32
        vm = lambda *shape: pltpu.VMEM(shape, f32)
        sems = lambda *shape: pltpu.SemaphoreType.DMA(shape)
        any_ = pl.BlockSpec(memory_space=pl.ANY)
        return pl.pallas_call(
            functools.partial(kernel, n, base),
            out_shape=(pltpu.VMEM(slab, f32), pltpu.VMEM(slab, f32)),
            in_specs=[any_] * 7,
            out_specs=(pl.BlockSpec(memory_space=pltpu.VMEM),) * 2,
            scratch_shapes=[
                pltpu.SMEM(contrast.shape, f32), vm(depth, height), vm(*slab),
                vm(*forward.shape), vm(*adjoint.shape),
                pltpu.VMEM(slab, jnp.int32), pltpu.VMEM(signs.shape, jnp.int32),
                vm(ITERS + 1, length + 6, depth, height),
                vm(*slab), vm(*slab), vm(*slab), vm(*slab), vm(*slab), vm(*slab),
                vm(ITERS, 2, *slab), vm(ITERS, *slab), vm(ITERS, *slab), vm(*slab),
                vm(*slab), vm(*slab),
                vm(ITERS, 3, depth, height), vm(ITERS, 2, depth, height),
                vm(ITERS, n, 3, rows, height), vm(ITERS, n, 2, rows, height),
                vm(ITERS, n, 2, rows, height), vm(ITERS, 2, depth, height),
                vm(8, height), vm(n, 8, height), vm(8, height), vm(8, height),
                sems(7), sems(ITERS + 1, 2, 2), sems(ITERS + 1, 2, 2),
                sems(ITERS, OWNERS), sems(ITERS), sems(ITERS, OWNERS), sems(ITERS),
                sems(ITERS, n), sems(ITERS), sems(1), sems(1), sems(n), sems(1),
            ],
            compiler_params=pltpu.CompilerParams(collective_id=0, has_side_effects=True),
        )(forward, adjoint, level, labels, signs, contrast, decay)

    return jax.shard_map(
        shards,
        mesh=mesh,
        in_specs=(
            P(None, ("corner", "gx"), None, None),
            P(None, ("corner", "gx"), None, None),
            P("gx", None, None),
            P("gx", None, None),
            P(None, "gx", None, None),
            P("corner"),
            P(),
        ),
        out_specs=(P(("corner", "gx"), None, None), P(("corner", "gx"), None, None)),
        check_vma=False,
    )
```

```python
import functools

import jax
import jax.numpy as jnp
from jax import lax
from jax.experimental import pallas as pl
from jax.experimental.pallas import tpu as pltpu
from jax.sharding import PartitionSpec as P

ITERS = 2
OWNERS = 4
MESH = pl.DeviceIdType.MESH

weno_eps = 1e-06
redist_step = 0.3
move_step = 0.5
cross_step = 0.3


def shift(a, step, axis):
    return pltpu.roll(a, (-step) % a.shape[axis], axis)


def weno_pair(d0, e0, e1, qm, q0, qp):
    c = 13.0 / 3.0
    r1, r2, r3 = e0 + (e0 + qm), e0 + e1, e1 + (e1 - qp)
    s1 = c * qm * qm + (r1 * r1 + 4.0 * weno_eps)
    s2 = c * q0 * q0 + (r2 * r2 + 4.0 * weno_eps)
    s3 = c * qp * qp + (r3 * r3 + 4.0 * weno_eps)
    t1, t2, t3 = s1 * s1, s2 * s2, s3 * s3
    m1, m2, m3 = t2 * t3, t1 * t3, t1 * t2
    six, three_1, three_3 = 6.0 * m2, 3.0 * m1, 3.0 * m3
    common = six * q0
    top = 1.5 * q0
    num_minus = m1 * qm + common + three_3 * (top - 0.5 * qp)
    num_plus = m3 * qp + common + three_1 * (top - 0.5 * qm)
    d3 = 3.0 * d0
    return (
        d3 + 1.5 * e0 + num_minus / (m1 + six + three_3),
        d3 - 1.5 * e1 + num_plus / (m3 + six + three_1),
    )


def rolled_sides(f, axis):
    d0 = shift(f, 1, axis) - f
    e0 = d0 - shift(d0, -1, axis)
    e1 = shift(e0, 1, axis)
    q0 = e1 - e0
    following, plus = weno_pair(d0, e0, e1, shift(q0, -1, axis), q0, shift(q0, 1, axis))
    return shift(following, -1, axis), plus


def slab_pass(length, ext, e, body):
    for r in range(0, ext.shape[2], 8):
        at = slice(r, r + 8)
        f = [ext[e, c, at] for c in range(length + 6)]
        d = [b - a for a, b in zip(f, f[1:])]
        s = [b - a for a, b in zip(d, d[1:])]
        q = [b - a for a, b in zip(s, s[1:])]
        minus = None
        for c in range(2, length + 3):
            following, plus = weno_pair(d[c], s[c - 1], s[c], q[c - 2], q[c - 1], q[c])
            if c > 2:
                body(c - 3, at, minus, plus)
            minus = following


def planes(length, body, unroll):
    if unroll == length:
        for i in range(length):
            body(i)
    else:
        def some(j, carry):
            for k in range(unroll):
                body(j * unroll + k)
            return carry

        lax.fori_loop(0, length // unroll, some, 0)


def kernel(
    n, base,
    fwd_hbm, adj_hbm, lvl_hbm, lab_hbm, sgn_hbm, contrast_hbm, decay_hbm,
    moved_out, speed_out,
    contrast, decay, base_size,
    fwd, adj, lab, sgn, ext, speed, kf, pf, kb, pb, kfc, cross, gain, kbc, u0, g_up, g_down,
    snd_c, snd_s, in_c, in_s, out_b, resp, pow_s, pow_in, pow_out, pow_res,
    load_sem, halo_send, halo_recv, c_send, c_recv, s_send, s_recv, r_send, r_recv,
    p_send, p_recv, q_send, q_recv,
):
    me = lax.axis_index("gx")
    corner = lax.axis_index("corner")
    length = lvl_hbm.shape[0]
    rows = lvl_hbm.shape[1] // OWNERS
    owner_no = (me - base) // 2
    is_owner = (me >= base) & (me < base + 2 * OWNERS) & (lax.rem(me - base + 2 * n, 2) == 0)

    def each(body):
        if n <= 16:
            for p in range(n):
                body(p)
        else:
            lax.fori_loop(0, n, lambda p, c: (body(p), c)[1], 0)

    loads = [
        pltpu.make_async_copy(src, dst, load_sem.at[k])
        for k, (src, dst) in enumerate((
            (lvl_hbm, ext.at[0, pl.ds(3, length)]), (sgn_hbm, sgn), (decay_hbm, decay),
            (contrast_hbm, contrast), (lab_hbm, lab), (fwd_hbm, fwd), (adj_hbm, adj)))
    ]
    for copy in loads:
        copy.start()

    barrier = pltpu.get_barrier_semaphore()

    def is_own(p):
        return (p >= base) & (p < base + 2 * OWNERS) & (lax.rem(p - base + 2 * n, 2) == 0)

    def greet(p):
        p = jnp.int32(p)
        meets = is_owner | is_own(p) | (p == me - 1) | (p == me + 1)

        @pl.when((p != me) & meets)
        def _():
            pl.semaphore_signal(barrier, inc=1, device_id=(corner, p), device_id_type=MESH)

    each(greet)

    @pl.when(me == 0)
    def _():
        for e in range(ITERS + 1):
            ext[e, 0:3] = jnp.zeros((3,) + ext.shape[2:], jnp.float32)

    @pl.when(me == n - 1)
    def _():
        for e in range(ITERS + 1):
            ext[e, length + 3 : length + 6] = jnp.zeros((3,) + ext.shape[2:], jnp.float32)

    def beside(p, inside):
        return (inside & jnp.logical_not(is_own(p))).astype(jnp.int32)

    met = jnp.where(is_owner, n - 1, OWNERS + beside(me - 1, me > 0) + beside(me + 1, me < n - 1))

    def halo_copy(e, side, part):
        planes = 1 if part == 0 else 2
        if side == 0:
            src, dst = (length + 2, 2) if part == 0 else (length, 0)
        else:
            src, dst = (3, length + 3) if part == 0 else (4, length + 4)
        return pltpu.make_async_remote_copy(
            src_ref=ext.at[e, pl.ds(src, planes)],
            dst_ref=ext.at[e, pl.ds(dst, planes)],
            send_sem=halo_send.at[e, side, part],
            recv_sem=halo_recv.at[e, side, part],
            device_id=(corner, me + 1 if side == 0 else me - 1),
            device_id_type=MESH,
        )

    def halo_start(e):
        for part in range(2):
            for side in range(2):
                @pl.when((me < n - 1) if side == 0 else (me > 0))
                def _():
                    halo_copy(e, side, part).start()

    def halo_wait(e, part):
        for side in range(2):
            @pl.when((me > 0) if side == 0 else (me < n - 1))
            def _():
                halo_copy(e, side, part).wait_recv()

    def to_owner(it, k, snd, dst, send, recv):
        owner = base + 2 * k
        src = snd.at[it, :, pl.ds(k * rows, rows), :]
        remote = pltpu.make_async_remote_copy(
            src_ref=src, dst_ref=dst.at[it, me], send_sem=send.at[it, k], recv_sem=recv.at[it],
            device_id=(corner, owner), device_id_type=MESH,
        )
        return owner, remote, pltpu.make_async_copy(src, dst.at[it, me], recv.at[it])

    def phase_one(it, snd, dst, send, recv):
        for k in range(OWNERS):
            owner, remote, local = to_owner(it, k, snd, dst, send, recv)

            @pl.when(me != owner)
            def _():
                remote.start()

            @pl.when(me == owner)
            def _():
                local.start()

    def pow_copy():
        return pltpu.make_async_remote_copy(
            src_ref=pow_s, dst_ref=pow_in.at[me], send_sem=p_send.at[0], recv_sem=p_recv.at[0],
            device_id=(corner, base), device_id_type=MESH,
        )

    def send_power():
        @pl.when(me != base)
        def _():
            pow_copy().start()

        @pl.when(me == base)
        def _():
            pltpu.make_async_copy(pow_s, pow_in.at[me], p_recv.at[0]).start()

    regions = contrast.shape[0]

    def raw_speed():
        acc = jnp.zeros(decay.shape, jnp.float32)
        for i in range(length):
            coupling = fwd[0, i] * adj[0, i]
            for k in range(1, fwd.shape[0]):
                coupling = coupling + fwd[k, i] * adj[k, i]
            labels = lab[i]
            material = jnp.zeros(labels.shape, jnp.float32)
            for region in range(regions):
                material = jnp.where(labels == region, contrast[region], material)
            value = material * coupling
            speed[i] = value
            acc = acc + value * value
        tile = acc[0:8]
        for k in range(8, acc.shape[0], 8):
            tile = tile + acc[k : k + 8]
        pow_s[...] = tile

    def plane_rates(it, which):
        for i in which:
            f = ext[it, i + 3]
            gx = 0.5 * (ext[it, i + 4] - ext[it, i + 2])
            gy = 0.5 * (shift(f, 1, 0) - shift(f, -1, 0))
            gz = 0.5 * (shift(f, 1, 1) - shift(f, -1, 1))
            inv = lax.rsqrt(jnp.maximum(gx * gx + gy * gy + gz * gz, 0.25))
            nx = gx * inv
            y = decay[...] * (0.5 + nx * nx)
            t = y * (1.0 - y * 0.5 * (1.0 - y * (1.0 / 3.0) * (1.0 - y * 0.25 * (1.0 - y * 0.2))))
            keep = 1.0 - t
            z = t * (2.0 - t)
            sx = sgn[0, i]
            third = jnp.float32(1.0 / 3.0)
            two = jnp.float32(2.0 / 3.0)
            one_ = jnp.float32(1.0)
            mf = jnp.where(sx > 0, one_, jnp.where(sx == 0, two, third))
            mb = jnp.where(sx < 0, one_, jnp.where(sx == 0, two, third))
            a9, a4 = jnp.float32(1.0 / 9.0), jnp.float32(4.0 / 9.0)
            vf = jnp.where(sx > 0, one_, jnp.where(sx == 0, a4, a9))
            vb = jnp.where(sx < 0, one_, jnp.where(sx == 0, a4, a9))
            kf[i] = keep * mf
            kb[i] = keep * mb
            pf[i] = jnp.sqrt((1.0 - vf) + vf * z)
            pb[i] = jnp.sqrt((1.0 - vb) + vb * z)
            cross[it, 0, i] = cross_step * jnp.abs(gy * inv) * sgn[1, i].astype(jnp.float32)
            cross[it, 1, i] = cross_step * jnp.abs(gz * inv) * sgn[2, i].astype(jnp.float32)

    def coefficients(it):
        halo_wait(it, 0)
        plane_rates(it, (0, length - 1))
        run = kf[0]
        kfc[0] = run
        for i in range(1, length):
            run = run * kf[i]
            kfc[i] = run
        snd_c[it, 0] = run
        g, k = pb[length - 1] * kfc[length - 1], kb[length - 1]
        gain[it, length - 1] = g
        kbc[it, length - 1] = k
        for i in range(length - 2, -1, -1):
            g = kb[i] * g + pb[i] * kfc[i]
            k = k * kb[i]
            gain[it, i] = g
            kbc[it, i] = k
        snd_c[it, 1] = k
        snd_c[it, 2] = g
        phase_one(it, snd_c, in_c, c_send, c_recv)

    def sweeps(it):
        w = pf[0] * speed[0]
        speed[0] = w
        for i in range(1, length):
            w = kf[i] * w + pf[i] * speed[i]
            speed[i] = w
        snd_s[it, 0] = w
        u = pb[length - 1] * w
        u0[length - 1] = u
        for i in range(length - 2, -1, -1):
            u = kb[i] * u + pb[i] * speed[i]
            u0[i] = u
        snd_s[it, 1] = u
        phase_one(it, snd_s, in_s, s_send, s_recv)

    def across(e):
        both = e == ITERS

        def body(i):
            f = ext[e, i + 3]
            pairs = (rolled_sides(f, 0), rolled_sides(f, 1))
            if both:
                rise = fall = None
                for minus, plus in pairs:
                    hi = jnp.maximum(jnp.maximum(minus, -plus), 0.0)
                    lo = jnp.minimum(jnp.minimum(minus, -plus), 0.0)
                    rise = hi * hi if rise is None else rise + hi * hi
                    fall = lo * lo if fall is None else fall + lo * lo
                g_up[i] = rise
                g_down[i] = fall
            else:
                up = ext[0, i + 3] >= 0.0
                total = None
                for minus, plus in pairs:
                    v = jnp.where(up, jnp.maximum(minus, -plus), jnp.maximum(-minus, plus))
                    v = jnp.maximum(v, 0.0)
                    total = v * v if total is None else total + v * v
                base_size[i] = total

        planes(length, body, 2)

    def along(e):
        both = e == ITERS
        if both:
            halo_wait(e, 0)
        halo_wait(e, 1)
        ninth = 1.0 / 9.0

        def body(i, at, minus, plus):
            if both:
                hi = jnp.maximum(jnp.maximum(minus, -plus), 0.0)
                lo = jnp.minimum(jnp.minimum(minus, -plus), 0.0)
                g_up[i, at] = jnp.sqrt((g_up[i, at] + hi * hi) * ninth + 1e-12)
                g_down[i, at] = jnp.sqrt((g_down[i, at] + lo * lo) * ninth + 1e-12)
            else:
                start = ext[0, i + 3, at]
                v = jnp.where(start >= 0.0, jnp.maximum(minus, -plus), jnp.maximum(-minus, plus))
                v = jnp.maximum(v, 0.0)
                size = jnp.sqrt((base_size[i, at] + v * v) * ninth + 1e-12)
                sign = start * lax.rsqrt(start * start + 1.0)
                ext[e + 1, i + 3, at] = ext[e, i + 3, at] - redist_step * sign * (size - 1.0)

        slab_pass(length, ext, e, body)
        if not both:
            halo_start(e + 1)

    def reply(it, p):
        src = out_b.at[it, p]
        dst = resp.at[it, :, pl.ds(pl.multiple_of(owner_no * rows, rows), rows), :]
        remote = pltpu.make_async_remote_copy(
            src_ref=src, dst_ref=dst, send_sem=r_send.at[it, p], recv_sem=r_recv.at[it],
            device_id=(corner, p), device_id_type=MESH,
        )
        return remote, pltpu.make_async_copy(src, dst, r_recv.at[it])

    def own(it):
        @pl.when(is_owner)
        def _():
            pltpu.make_async_copy(in_c.at[it], in_c.at[it], c_recv.at[it]).wait()
            pltpu.make_async_copy(in_s.at[it], in_s.at[it], s_recv.at[it]).wait()
            zero = jnp.zeros(in_s.shape[3:], jnp.float32)

            def ahead(p, w):
                out_b[it, p, 0] = w
                return in_c[it, p, 0] * w + in_s[it, p, 0]

            def back(turn, u):
                p = n - 1 - turn
                out_b[it, p, 1] = u
                return in_c[it, p, 1] * u + (in_c[it, p, 2] * out_b[it, p, 0] + in_s[it, p, 1])

            lax.fori_loop(0, n, ahead, zero, unroll=n <= 16)
            lax.fori_loop(0, n, back, zero, unroll=n <= 16)

            def send(p):
                remote, local = reply(it, p)

                @pl.when(p != me)
                def _():
                    remote.start()

                @pl.when(p == me)
                def _():
                    local.start()

            each(send)

    def pow_reply(p):
        remote = pltpu.make_async_remote_copy(
            src_ref=pow_out, dst_ref=pow_res, send_sem=q_send.at[p], recv_sem=q_recv.at[0],
            device_id=(corner, p), device_id_type=MESH,
        )
        return remote, pltpu.make_async_copy(pow_out, pow_res, q_recv.at[0])

    def own_power():
        @pl.when(me == base)
        def _():
            pltpu.make_async_copy(pow_in, pow_in, p_recv.at[0]).wait()
            pow_out[...] = lax.fori_loop(
                0, n, lambda p, acc: acc + pow_in[p], jnp.zeros(pow_out.shape, jnp.float32)
            )

            def send(p):
                remote, local = pow_reply(p)

                @pl.when(p != me)
                def _():
                    remote.start()

                @pl.when(p == me)
                def _():
                    local.start()

            each(send)

    def finish(it, body):
        pltpu.make_async_copy(resp.at[it], resp.at[it], r_recv.at[it]).wait()

        for i in range(length):
            s = u0[i] + gain[it, i] * resp[it, 0] + kbc[it, i] * resp[it, 1]
            cy, cz = cross[it, 0, i], cross[it, 1, i]
            near_y = jnp.where(cy > 0.0, shift(s, -1, 0), shift(s, 1, 0))
            near_z = jnp.where(cz > 0.0, shift(s, -1, 1), shift(s, 1, 1))
            body(i, s - (jnp.abs(cy) * (s - near_y) + jnp.abs(cz) * (s - near_z)))

    def keep_speed(i, s):
        speed[i] = s

    inner = range(1, length - 1)
    for copy in loads[:3]:
        copy.wait()
    plane_rates(0, inner)
    pl.semaphore_wait(barrier, met)
    halo_start(0)
    for copy in loads[3:]:
        copy.wait()
    raw_speed()
    across(0)
    coefficients(0)
    sweeps(0)
    send_power()
    along(0)
    plane_rates(1, inner)
    across(1)
    own(0)
    own_power()
    coefficients(1)
    along(1)
    across(2)
    finish(0, keep_speed)
    sweeps(1)
    along(2)
    own(1)

    pltpu.make_async_copy(pow_res, pow_res, q_recv.at[0]).wait()
    cells = length * decay.shape[0] * decay.shape[1] * n
    total = jnp.sum(pow_res[...], keepdims=True)
    scale = lax.rsqrt(total * (1.0 / cells) + 1e-06)

    def emit(i, s):
        s = s * scale
        speed_out[i] = s
        size = jnp.where(s >= 0.0, g_up[i], g_down[i])
        moved_out[i] = ext[ITERS, i + 3] - move_step * s * size

    finish(ITERS - 1, emit)
    for e in range(ITERS + 1):
        for part in range(2):
            for side in range(2):
                @pl.when((me < n - 1) if side == 0 else (me > 0))
                def _():
                    halo_copy(e, side, part).wait_send()

    for it in range(ITERS):
        for k in range(OWNERS):
            for args in ((snd_c, in_c, c_send, c_recv), (snd_s, in_s, s_send, s_recv)):
                owner, remote, _ = to_owner(it, k, *args)

                @pl.when(me != owner)
                def _():
                    remote.wait_send()

    @pl.when(me != base)
    def _():
        pow_copy().wait_send()

    @pl.when(is_owner)
    def _():
        for it in range(ITERS):
            def done(p):
                @pl.when(p != me)
                def _():
                    reply(it, p)[0].wait_send()

            each(done)

    @pl.when(me == base)
    def _():
        def done(p):
            @pl.when(p != me)
            def _():
                pow_reply(p)[0].wait_send()

        each(done)


def solution(mesh):
    n = mesh.shape["gx"]
    base = n // 2 - OWNERS + 1

    def shards(forward, adjoint, level, labels, signs, contrast, decay):
        slab = level.shape
        length, depth, height = slab
        rows = depth // OWNERS
        f32 = jnp.float32
        vm = lambda *shape: pltpu.VMEM(shape, f32)
        sems = lambda *shape: pltpu.SemaphoreType.DMA(shape)
        any_ = pl.BlockSpec(memory_space=pl.ANY)
        return pl.pallas_call(
            functools.partial(kernel, n, base),
            out_shape=(pltpu.VMEM(slab, f32), pltpu.VMEM(slab, f32)),
            in_specs=[any_] * 7,
            out_specs=(pl.BlockSpec(memory_space=pltpu.VMEM),) * 2,
            scratch_shapes=[
                pltpu.SMEM(contrast.shape, f32), vm(depth, height), vm(*slab),
                vm(*forward.shape), vm(*adjoint.shape),
                pltpu.VMEM(slab, jnp.int32), pltpu.VMEM(signs.shape, jnp.int32),
                vm(ITERS + 1, length + 6, depth, height),
                vm(*slab), vm(*slab), vm(*slab), vm(*slab), vm(*slab), vm(*slab),
                vm(ITERS, 2, *slab), vm(ITERS, *slab), vm(ITERS, *slab), vm(*slab),
                vm(*slab), vm(*slab),
                vm(ITERS, 3, depth, height), vm(ITERS, 2, depth, height),
                vm(ITERS, n, 3, rows, height), vm(ITERS, n, 2, rows, height),
                vm(ITERS, n, 2, rows, height), vm(ITERS, 2, depth, height),
                vm(8, height), vm(n, 8, height), vm(8, height), vm(8, height),
                sems(7), sems(ITERS + 1, 2, 2), sems(ITERS + 1, 2, 2),
                sems(ITERS, OWNERS), sems(ITERS), sems(ITERS, OWNERS), sems(ITERS),
                sems(ITERS, n), sems(ITERS), sems(1), sems(1), sems(n), sems(1),
            ],
            compiler_params=pltpu.CompilerParams(collective_id=0, has_side_effects=True),
        )(forward, adjoint, level, labels, signs, contrast, decay)

    return jax.shard_map(
        shards,
        mesh=mesh,
        in_specs=(
            P(None, ("corner", "gx"), None, None),
            P(None, ("corner", "gx"), None, None),
            P("gx", None, None),
            P("gx", None, None),
            P(None, "gx", None, None),
            P("corner"),
            P(),
        ),
        out_specs=(P(("corner", "gx"), None, None), P(("corner", "gx"), None, None)),
        check_vma=False,
    )
```
